128 devices in a mesh: seq: 4 (over z_lo, core), ctx: 32 (over y, x, z_hi).
Axes of the slice: x: 4, y: 4, z: 4 (z_hi: 2, z_lo: 2; z = z_hi * 2 + z_lo), core: 2. Of those that a mesh axis runs over, the one named last changes fastest.
Arguments:
- hidden: bfloat16 [131072, 7168], P(('seq', 'ctx')), may hold values from -24 to 24
- router_weight: bfloat16 [7168, 256], replicated, may hold values from -0.0625 to 0.0625
- expert_index: int32 [131072, 8], P(('seq', 'ctx')), may hold values from 0 to 255, all different within a row
- lengths: int32 [4], P('seq'), may hold values from 16384 to 32768
Outputs:
- router_grad: float32 [7168, 256], P('ctx')
- balance: float32 [4], P('seq')
The draws below stay inside these ranges and needn't reach their ends.
Inputs may be any that keep to these rules, and one draw needn't show every extreme that they name: A sequence's valid tokens are its first lengths[s] slots, the rest are padding. `expert_index`: each row names 8 different experts.
All inputs are finite; a program needn't handle non-finite values.
Results may differ from the reference program's by a relative error of at most 0.0003.
Values sent between devices are 32-bit elements; how exact they have to be, the bound alone decides.
A program may use at most 128 MiB of HBM per device.

```python
import jax
import jax.numpy as jnp
from jax import lax

D = 7168
E = 256
TOPK = 8
LEN = 32768
SEQS = 4
TOKENS = 131072


def place_ends(values, rng, least, largest):
    extent = values.shape
    place = [jax.random.randint(jax.random.fold_in(rng, axis), (), 0, extent[axis]) for axis in range(len(extent))]
    values = values.at[tuple(place)].set(least)
    longest = extent.index(max(extent))
    place[longest] = (place[longest] + 1) % extent[longest]
    return values.at[tuple(place)].set(largest)


def strengthened(array, own_key, source, target, blocks, factor):
    def block_of(axis_at):
        return (jnp.arange(array.shape[axis_at]) // (array.shape[axis_at] // blocks)).reshape((-1,) + (1,) * (array.ndim - 1 - axis_at))

    near = jax.random.permutation(own_key, blocks)[block_of(target)]
    second = (block_of(target) + blocks // 2) % blocks
    return jnp.where((block_of(source) == near) | (block_of(source) == second), factor * array, array)


def block_levels(own_key, dims, shards, smallest, largest):
    level = 1.0
    for axis_at, blocks in shards:
        heights = jax.random.uniform(jax.random.fold_in(jax.random.fold_in(own_key, 6), axis_at), (blocks,), jnp.float32, smallest / len(shards), largest / len(shards))
        level = level * jnp.repeat(jnp.exp(heights), dims[axis_at] // blocks).reshape((-1,) + (1,) * (len(dims) - 1 - axis_at))
    return level


def distinct(rng, rows, amount, top, lift):
    ranking = jax.random.permutation(jax.random.fold_in(rng, 1), amount)
    boost = ranking
    for power in range(3):
        boost = boost * boost // amount
    boost = boost * lift // amount
    lots = jax.random.randint(jax.random.fold_in(rng, 2), (rows, amount), 0, 4096) + boost
    sure = jax.random.permutation(jax.random.fold_in(rng, 3), rows)[jnp.arange(amount) % rows]
    lots = jnp.where(jnp.arange(rows)[:, None] == sure[None, :], 1 << 14, lots)
    priority = lots * amount + jnp.arange(amount)
    return lax.top_k(priority.astype(jnp.int32), top)[1].astype(jnp.int32)


def normal_values(key, dims, spread, most, cuts=(), kind=jnp.bfloat16):
    result = jax.random.normal(key, dims, jnp.float32) * spread
    if len(cuts) > 0:
        result = block_levels(key, dims, cuts, -0.22, 0.18) * result
    return jnp.clip(result, min=-most, max=most).astype(kind)


def heavy_noise(key, dims, spread, most, pieces, heavy, kind=jnp.bfloat16):
    array = spread * jax.random.normal(key, dims, jnp.float32)
    if pieces:
        array = array * block_levels(key, dims, pieces, -0.22, 0.18)
    return jnp.clip(strengthened(array, jax.random.fold_in(key, 3), *heavy), -most, most).astype(kind)


def setup_inputs(seed: int = 0) -> dict:
    keys = jax.random.split(jax.random.key(seed), 5)
    return {
        "hidden": heavy_noise(keys[0], (TOKENS, D), 1.0, 24.0, ((0, 128),), (0, 1, 128, 5.5)),
        "router_weight": normal_values(keys[1], (D, E), D ** -0.5, 0.0625),
        "expert_index": distinct(keys[2], TOKENS, E, TOPK, 256),
        "lengths": place_ends(jax.random.randint(keys[3], (SEQS,), LEN // 2, LEN + 1), jax.random.fold_in(keys[3], 1), LEN // 2, LEN).astype(jnp.int32),
    }


loss_scale = 65536.0


def reference(hidden, router_weight, expert_index, lengths):
    hidden_all = hidden.reshape(SEQS, LEN, D)
    index_all = expert_index.reshape(SEQS, LEN, TOPK)

    def one_sequence(packed):
        hidden_seq, index_seq, length_seq = packed
        tokens_live = length_seq.astype(jnp.float32)
        logits = jnp.dot(hidden_seq, router_weight, preferred_element_type=jnp.float32)
        scores = jax.nn.sigmoid(logits)
        row_total = jnp.sum(scores, axis=1, keepdims=True)
        share_of = scores / row_total
        positions = jnp.arange(LEN, dtype=jnp.int32)
        valid_mask = (positions < length_seq.astype(jnp.int32)).astype(jnp.float32)
        expert_ids = jnp.arange(E, dtype=jnp.int32)
        expert_hits = jnp.sum((index_seq[:, :, None] == expert_ids).astype(jnp.float32), axis=1)
        counts = jnp.sum(valid_mask[:, None] * expert_hits, axis=0)
        score_sum = jnp.sum(valid_mask[:, None] * share_of, axis=0)
        fraction = E * counts / (TOPK * tokens_live)
        mean_score = score_sum / tokens_live
        balance = jnp.sum(fraction * mean_score)
        weights = loss_scale * fraction / tokens_live
        weighted = jnp.sum(weights * share_of, axis=1, keepdims=True)
        grad_logits = (weights - weighted) / row_total * scores * (1.0 - scores) * valid_mask[:, None]
        grad_seq = lax.dot_general(hidden_seq.astype(jnp.float32), grad_logits, (((0,), (0,)), ((), ())), precision=lax.Precision.HIGHEST, preferred_element_type=jnp.float32)
        return balance, grad_seq

    balance, grad_stack = lax.map(one_sequence, (hidden_all, index_all, lengths))
    return jnp.sum(grad_stack, axis=0), balance
```

```python
import jax
import jax.numpy as jnp
from jax import lax
from jax.experimental import pallas as pl
from jax.experimental.pallas import tpu as pltpu
from jax.sharding import PartitionSpec as P

D = 7168
E = 256
TOPK = 8
ROWS = 1024
BLOCK = 224
HALF = BLOCK // 2
CHUNK = 4 * BLOCK
LOSS_SCALE = 65536.0
MESH = pl.DeviceIdType.MESH

TILES = (3, 2, 2, 3, 2, 2)
OFFSET = (0, 24, 40, 56, 80, 96)
LEAD = ((64,), (4, 8, 2), (2, 8, 4), (8, 8), (4, 8, 2), (2, 8, 4))

HCH = 4
HROWS = ROWS // HCH


def place(s, j, b):
    return (
        (j * 8 + b,),
        (j % 4, b, j // 4),
        (j % 2, b, j // 2),
        (b, j),
        (b % 4, j, b // 4),
        (b % 2, j, b // 2),
    )[s]


def first_send(s, j):
    return (
        (pl.ds(j * 8, 8),),
        (j % 4, slice(None), j // 4),
        (j % 2, slice(None), j // 2),
        (pl.ds(4, 4), j),
        (pl.ds(2, 2), j, slice(None)),
        (1, j, slice(None)),
    )[s]


def span(lead, start, size):
    inner = 1
    for n in lead[1:]:
        inner *= n
    if size >= inner or len(lead) == 1:
        return (pl.ds(start // inner, size // inner),) + (slice(None),) * (len(lead) - 1)
    return (start // inner,) + span(lead[1:], start % inner, size)


def kernel(hid, wt, eidx, lens, out, bal, *scratch):
    (h, w, idx, length, share, coef, ghi, glo, own, snd, got) = scratch[:11]
    acc, rb = scratch[11:17], scratch[17:23]
    (fin, ar, in_sem, d2d_s, d2d_r, cube_s, cube_r, ar_s, ar_r, fin_s, fin_r) = scratch[23:]

    seq, ctx = lax.axis_index("seq"), lax.axis_index("ctx")
    core, zlo = seq % 2, seq // 2
    zh, x, y = ctx % 2, (ctx // 2) % 4, ctx // 8

    def device(y_, x_, zh_, zlo_, core_):
        return (zlo_ * 2 + core_, (y_ * 4 + x_) * 2 + zh_)

    cube = (
        device(3 - y, x, zh, zlo, core),
        device(y + 1 - 2 * (y % 2), x, zh, zlo, core),
        device(y, 3 - x, zh, zlo, core),
        device(y, x + 1 - 2 * (x % 2), zh, zlo, core),
        device(y, x, 1 - zh, 1 - zlo, core),
        device(y, x, zh, 1 - zlo, core),
    )
    other = device(y, x, zh, zlo, 1 - core)
    cross = device(y, x, zh, 1 - zlo, 1 - core)
    ring_x = [device(y, (x + d) % 4, zh, zlo, core) for d in (1, 2, 3)]
    ring_y = [device((y + d) % 4, x, zh, zlo, core) for d in (1, 2, 3)]
    pair_z = [device(y, x, 1 - zh, zlo, core)]
    stages = ((ring_x, x), (ring_y, y), (pair_z, zh))

    barrier = pltpu.get_barrier_semaphore()
    greeted = ring_x + ring_y + pair_z + [cube[4], cube[5], other, cross]
    for peer in greeted:
        pl.semaphore_signal(barrier, inc=1, device_id=peer, device_id_type=MESH)

    load_len = pltpu.make_async_copy(lens, length, in_sem.at[0])
    load_idx = pltpu.make_async_copy(eidx, idx, in_sem.at[1])
    load_w = pltpu.make_async_copy(wt, w, in_sem.at[2])
    load_h = [
        pltpu.make_async_copy(hid.at[pl.ds(c * HROWS, HROWS)], h.at[pl.ds(c * HROWS, HROWS)], in_sem.at[3 + c])
        for c in range(HCH)
    ]
    load_len.start()
    load_idx.start()
    load_w.start()
    for c in range(HCH):
        load_h[c].start()

    load_len.wait()
    load_idx.wait()
    live = length[0]
    first = ctx * ROWS

    def count(i, total):
        r0 = pl.multiple_of(i * 64, 64)
        block = idx[pl.ds(r0, 64), :]
        position = first + r0 + lax.broadcasted_iota(jnp.int32, block.shape, 0)
        block = jnp.where(position < live, block, -1)
        experts = lax.broadcasted_iota(jnp.int32, (64, E), 1)
        hits = jnp.zeros((64, E), jnp.float32)
        for k in range(TOPK):
            hits = hits + jnp.where(block[:, k : k + 1] == experts, 1.0, 0.0)
        return total + hits.reshape(8, 8, E).sum(axis=0)

    counts = lax.fori_loop(0, ROWS // 64, count, jnp.zeros((8, E), jnp.float32))

    def ar_copy(kind, stage, peer, where):
        return pltpu.make_async_remote_copy(
            src_ref=ar.at[(kind, stage) + where],
            dst_ref=ar.at[(kind, stage) + where],
            send_sem=ar_s.at[kind, stage],
            recv_sem=ar_r.at[kind, stage],
            device_id=peer,
            device_id_type=MESH,
        )

    def ar_send(kind, stage, value):
        peers, mine = stages[stage]
        ar[kind, stage, mine] = value
        for peer in peers:
            ar_copy(kind, stage, peer, (mine,)).start()

    def ar_wait(kind, stage):
        peers, _ = stages[stage]
        n = len(peers)
        ar_copy(kind, stage, peers[0], (pl.ds(0, n),)).wait()
        total = ar[kind, stage, 0]
        for i in range(1, n + 1):
            total = total + ar[kind, stage, i]
        return total

    pl.semaphore_wait(barrier, len(greeted))
    ar_send(0, 0, counts)

    load_w.wait()
    score_sum = jnp.zeros((8, E), jnp.float32)
    for c in range(HCH):
        rows = pl.ds(c * HROWS, HROWS)
        load_h[c].wait()
        logits = jnp.dot(h[rows, :], w[...], preferred_element_type=jnp.float32)
        scores = jax.nn.sigmoid(logits)
        row_total = jnp.sum(scores, axis=1, keepdims=True)
        position = first + c * HROWS + lax.broadcasted_iota(jnp.int32, (HROWS, 1), 0)
        valid = jnp.where(position < live, 1.0, 0.0)
        part = scores / row_total
        share[rows, :] = part
        coef[rows, :] = part * (1.0 - scores) * valid
        score_sum = score_sum + (part * valid).reshape(HROWS // 8, 8, E).sum(axis=0)
        if c == 0:
            counts = ar_wait(0, 0)
            ar_send(0, 1, counts)
        if c == 2:
            counts = ar_wait(0, 1)
            ar_send(0, 2, counts)
    counts = ar_wait(0, 2)
    ar_send(1, 0, score_sum)

    tokens = live.astype(jnp.float32)
    fraction = E * jnp.sum(counts, axis=0, keepdims=True) / (TOPK * tokens)
    weights = LOSS_SCALE * fraction / tokens
    for c in range(HCH):
        rows = pl.ds(c * HROWS, HROWS)
        weighted = jnp.sum(weights * share[rows, :], axis=1, keepdims=True)
        grad = (weights - weighted) * coef[rows, :]
        high = grad.astype(jnp.bfloat16)
        low = (grad - high.astype(jnp.float32)).astype(jnp.bfloat16)
        for e in range(2):
            columns = pl.ds(pl.multiple_of(((core + e) % 2) * 128, 128), 128)
            ghi[rows, columns] = high[:, e * 128 : (e + 1) * 128]
            glo[rows, columns] = low[:, e * 128 : (e + 1) * 128]

    def d2d(j):
        return pltpu.make_async_remote_copy(
            src_ref=snd.at[j], dst_ref=got.at[j], send_sem=d2d_s.at[j], recv_sem=d2d_r.at[j],
            device_id=other, device_id_type=MESH,
        )

    def halving(s, k, where):
        return pltpu.make_async_remote_copy(
            src_ref=acc[s].at[where], dst_ref=rb[s].at[where], send_sem=cube_s.at[s, k], recv_sem=cube_r.at[s, k],
            device_id=cube[(s + k) % 6], device_id_type=MESH,
        )

    yhi, xhi = y // 2, x // 2
    ylo, xlo = (yhi + y) % 2, (xhi + x) % 2
    v = (zh + zlo) % 2

    def multiply(j):
        y_hi = (yhi + j // 4) % 2
        y_at = 2 * y_hi + (y_hi + ylo + (j // 2) % 2) % 2
        x_hi = (xhi + j) % 2
        start = (y_at * 2 + x_hi) * CHUNK
        for m in range(CHUNK // 128):
            part = h[:, pl.ds(pl.multiple_of(start + m * 128, 128), 128)]
            dims = (((0,), (0,)), ((), ()))
            made = lax.dot_general(part, ghi[...], dims, preferred_element_type=jnp.float32)
            made = made + lax.dot_general(part, glo[...], dims, preferred_element_type=jnp.float32)
            at = m * 128
            while at < (m + 1) * 128:
                to = min((at // HALF + 1) * HALF, (m + 1) * 128)
                piece = at // HALF
                b1 = (x_hi + piece // 4 + xlo) % 2
                b2 = (piece // 2 % 2 + zh) % 2
                b3 = (piece % 2 + v) % 2
                b = b1 * 4 + b2 * 2 + b3
                lo, size = at - piece * HALF, to - at
                own[j, b, lo : lo + size] = made[at - m * 128 : to - m * 128, :128]
                snd[j, b, lo : lo + size] = made[at - m * 128 : to - m * 128, 128:]
                at = to
        d2d(j).start()

    def gather(j):
        d2d(j).wait_recv()
        for b in range(8):
            total = own[j, b] + got[j, b]
            for s in range(6):
                acc[s][place(s, j, b)] = total[OFFSET[s] : OFFSET[s] + 8 * TILES[s]]
        for s in range(3, 6):
            halving(s, 0, first_send(s, j)).start()
        for s, bit in ((0, j // 4), (1, (j // 2) % 2), (2, j % 2)):

            @pl.when(bit == 1)
            def _(s=s):
                halving(s, 0, first_send(s, j)).start()

    def step(i, carry):
        @pl.when(i < 8)
        def _():
            multiply(7 - i)

        @pl.when(i > 0)
        def _():
            gather(8 - i)

        return carry

    lax.fori_loop(0, 9, step, 0)

    score_sum = ar_wait(1, 0)
    ar_send(1, 1, score_sum)

    for k in range(6):
        n = 32 >> k
        for s in range(6):
            halving(s, k, span(LEAD[s], n, n)).wait_recv()
            low_half, high_half = span(LEAD[s], 0, n), span(LEAD[s], n, n)
            acc[s][low_half] = acc[s][low_half] + rb[s][high_half]
            if k < 5:
                halving(s, k + 1, span(LEAD[s], n // 2, n // 2)).start()
        if k == 2:
            score_sum = ar_wait(1, 1)
            ar_send(1, 2, score_sum)

    for s in range(6):
        zero = (0,) * len(LEAD[s])
        fin[core, v, OFFSET[s] : OFFSET[s] + 8 * TILES[s]] = acc[s][zero]

    last = [
        pltpu.make_async_remote_copy(
            src_ref=fin.at[core, v], dst_ref=fin.at[core, v], send_sem=fin_s.at[i], recv_sem=fin_r.at[i],
            device_id=peer, device_id_type=MESH,
        )
        for i, peer in enumerate((cube[5], cross, other))
    ]
    for copy in last:
        copy.start()

    score_sum = ar_wait(1, 2)
    mean_score = jnp.sum(score_sum, axis=0, keepdims=True) / tokens
    bal[0] = jnp.sum(fraction * mean_score)

    for k in range(6):
        for s in range(6):
            halving(s, k, span(LEAD[s], 32 >> k, 32 >> k)).wait_send()
    for j in range(8):
        d2d(j).wait_send()
    for copy in last:
        copy.wait()
    for e in range(2):
        for half in range(2):
            out[half * HALF : (half + 1) * HALF, e * 128 : (e + 1) * 128] = fin[e, half]


def solution(mesh):
    def shards(hidden, router_weight, expert_index, lengths):
        any_space = pl.BlockSpec(memory_space=pl.ANY)
        pieces = [lead + (8 * t, 128) for lead, t in zip(LEAD, TILES)]
        return pl.pallas_call(
            kernel,
            out_shape=(jax.ShapeDtypeStruct((BLOCK, E), jnp.float32), jax.ShapeDtypeStruct((1,), jnp.float32)),
            in_specs=[any_space] * 4,
            out_specs=(pl.BlockSpec(memory_space=pltpu.VMEM), pl.BlockSpec(memory_space=pltpu.SMEM)),
            scratch_shapes=[
                pltpu.VMEM((ROWS, D), jnp.bfloat16),
                pltpu.VMEM((D, E), jnp.bfloat16),
                pltpu.VMEM((ROWS, TOPK), jnp.int32),
                pltpu.SMEM((1,), jnp.int32),
                pltpu.VMEM((ROWS, E), jnp.float32),
                pltpu.VMEM((ROWS, E), jnp.float32),
                pltpu.VMEM((ROWS, E), jnp.bfloat16),
                pltpu.VMEM((ROWS, E), jnp.bfloat16),
                pltpu.VMEM((8, 8, HALF, 128), jnp.float32),
                pltpu.VMEM((8, 8, HALF, 128), jnp.float32),
                pltpu.VMEM((8, 8, HALF, 128), jnp.float32),
                *[pltpu.VMEM(p, jnp.float32) for p in pieces],
                *[pltpu.VMEM(p, jnp.float32) for p in pieces],
                pltpu.VMEM((2, 2, HALF, 128), jnp.float32),
                pltpu.VMEM((2, 3, 4, 8, E), jnp.float32),
                pltpu.SemaphoreType.DMA((3 + HCH,)),
                pltpu.SemaphoreType.DMA((8,)),
                pltpu.SemaphoreType.DMA((8,)),
                pltpu.SemaphoreType.DMA((6, 6)),
                pltpu.SemaphoreType.DMA((6, 6)),
                pltpu.SemaphoreType.DMA((2, 3)),
                pltpu.SemaphoreType.DMA((2, 3)),
                pltpu.SemaphoreType.DMA((3,)),
                pltpu.SemaphoreType.DMA((3,)),
            ],
            compiler_params=pltpu.CompilerParams(
                collective_id=0, has_side_effects=True, vmem_limit_bytes=60 * 1024 * 1024
            ),
        )(hidden, router_weight, expert_index, lengths)

    return jax.shard_map(
        shards,
        mesh=mesh,
        in_specs=(P(("seq", "ctx"), None), P(), P(("seq", "ctx"), None), P("seq")),
        out_specs=(P("ctx", None), P("seq")),
        check_vma=False,
    )
```

```python
import jax
import jax.numpy as jnp
from jax import lax
from jax.experimental import pallas as pl
from jax.experimental.pallas import tpu as pltpu
from jax.sharding import PartitionSpec as P

D = 7168
E = 256
TOPK = 8
ROWS = 1024
BLOCK = 224
HALF = BLOCK // 2
CHUNK = 4 * BLOCK
LOSS_SCALE = 65536.0
MESH = pl.DeviceIdType.MESH

SETS = (((0, 2), (1, 1), (2, 1), (3, 2), (4, 1), (5, 1)), ((0, 1), (1, 1), (2, 1), (3, 1), (4, 1), (5, 1)))
PIECES = tuple((t, n) for pieces in SETS for t, n in pieces)
TURN = tuple(t for t, _ in PIECES)
TILES = tuple(n for _, n in PIECES)
OFFSET = tuple(8 * sum(TILES[:p]) for p in range(len(PIECES)))
NP = len(PIECES)
SET_OF = (range(0, 6), range(6, 12))
SET_ROWS = ((0, 64), (64, 48))

HCH = 4
HROWS = ROWS // HCH
STRIP = 64


def turn(i, t):
    return (i, (i % 4) * 2 + i // 4, (i % 2) * 4 + i // 2)[t]


def place(p, j, b):
    t = TURN[p]
    return (turn(j, t), b) if t < 3 else (turn(b, t - 3), j)


def dimension(p, k):
    t = TURN[p]
    return (t + k) % 3 if t < 3 else 3 + (t + k) % 3


def kernel(hid, wt, eidx, lens, out, bal, *scratch):
    (h, w, idx, length, share, coef, ghi, glo, own, snd, got) = scratch[:11]
    acc, rb = scratch[11 : 11 + NP], scratch[11 + NP : 11 + 2 * NP]
    (fin, ar, in_sem, d2d_s, d2d_r, cube_s, cube_r, ar_s, ar_r, fin_s, fin_r) = scratch[11 + 2 * NP :]

    seq, ctx = lax.axis_index("seq"), lax.axis_index("ctx")
    core, zlo = seq % 2, seq // 2
    zh, x, y = ctx % 2, (ctx // 2) % 4, ctx // 8

    def device(y_, x_, zh_, zlo_, core_):
        return (zlo_ * 2 + core_, (y_ * 4 + x_) * 2 + zh_)

    def across(bits):
        y_, x_, zh_, zlo_ = y, x, zh, zlo
        if bits & 32:
            y_ = 3 - y_
        if bits & 16:
            y_ = y_ + 1 - 2 * (y_ % 2)
        if bits & 8:
            x_ = 3 - x_
        if bits & 4:
            x_ = x_ + 1 - 2 * (x_ % 2)
        if bits & 2:
            zh_, zlo_ = 1 - zh_, 1 - zlo_
        if bits & 1:
            zlo_ = 1 - zlo_
        return device(y_, x_, zh_, zlo_, core)

    cube = [across(32 >> d) for d in range(6)]
    far = ([across(r) for r in range(8)], [across(8 * r) for r in range(8)])
    other = device(y, x, zh, zlo, 1 - core)
    cross = device(y, x, zh, 1 - zlo, 1 - core)
    ring_x = [device(y, (x + d) % 4, zh, zlo, core) for d in (1, 2, 3)]
    ring_y = [device((y + d) % 4, x, zh, zlo, core) for d in (1, 2, 3)]
    pair_z = [device(y, x, 1 - zh, zlo, core)]
    stages = ((ring_x, x), (ring_y, y), (pair_z, zh))

    barrier = pltpu.get_barrier_semaphore()
    greeted = [across(r) for r in range(1, 8)] + [across(8 * r) for r in range(1, 8)] + pair_z + [other, cross]
    greeted += [device(y, (x + 2) % 4, zh, zlo, core), device((y + 2) % 4, x, zh, zlo, core)]
    for peer in greeted:
        pl.semaphore_signal(barrier, inc=1, device_id=peer, device_id_type=MESH)

    load_len = pltpu.make_async_copy(lens, length, in_sem.at[0])
    load_idx = pltpu.make_async_copy(eidx, idx, in_sem.at[1])
    load_w = [
        pltpu.make_async_copy(
            wt.at[:, pl.ds(pl.multiple_of(((core + e) % 2) * 128, 128), 128)], w.at[:, e * 128 : (e + 1) * 128],
            in_sem.at[2 + e],
        )
        for e in range(2)
    ]
    load_h = [
        pltpu.make_async_copy(hid.at[pl.ds(c * HROWS, HROWS)], h.at[pl.ds(c * HROWS, HROWS)], in_sem.at[4 + c])
        for c in range(HCH)
    ]
    load_len.start()
    load_idx.start()
    for e in range(2):
        load_w[e].start()
    for c in range(HCH):
        load_h[c].start()

    load_len.wait()
    load_idx.wait()
    live = length[0]
    first = ctx * ROWS

    hits = jnp.zeros((E, 128), jnp.float32)
    experts = (lax.broadcasted_iota(jnp.int32, (E, 128), 0) + core * 128) % E
    for i in range(ROWS // 128):
        block = idx[:, i * 128 : (i + 1) * 128]
        position = first + i * 128 + lax.broadcasted_iota(jnp.int32, block.shape, 1)
        block = jnp.where(position < live, block, -1)
        for k in range(TOPK):
            hits = hits + jnp.where(block[k : k + 1, :] == experts, 1.0, 0.0)
    counts = lax.dot_general(
        jnp.ones((8, 128), jnp.bfloat16), hits.astype(jnp.bfloat16), (((1,), (1,)), ((), ())),
        preferred_element_type=jnp.float32,
    )

    def ar_copy(kind, stage, peer, where):
        return pltpu.make_async_remote_copy(
            src_ref=ar.at[(kind, stage) + where],
            dst_ref=ar.at[(kind, stage) + where],
            send_sem=ar_s.at[kind, stage],
            recv_sem=ar_r.at[kind, stage],
            device_id=peer,
            device_id_type=MESH,
        )

    def ar_send(kind, stage, value):
        peers, mine = stages[stage]
        ar[kind, stage, mine] = value
        for peer in peers:
            ar_copy(kind, stage, peer, (mine,)).start()

    def ar_wait(kind, stage):
        peers, _ = stages[stage]
        n = len(peers)
        ar_copy(kind, stage, peers[0], (pl.ds(0, n),)).wait()
        total = ar[kind, stage, 0]
        for i in range(1, n + 1):
            total = total + ar[kind, stage, i]
        return total

    pl.semaphore_wait(barrier, len(greeted))
    ar_send(0, 0, counts)

    for e in range(2):
        load_w[e].wait()
    score_sum = jnp.zeros((8, E), jnp.float32)
    for c in range(HCH):
        rows = pl.ds(c * HROWS, HROWS)
        load_h[c].wait()
        share[rows, :] = jnp.dot(h[rows, :], w[...], preferred_element_type=jnp.float32)
        for r0 in range(c * HROWS, (c + 1) * HROWS, STRIP):
            rows = pl.ds(r0, STRIP)
            scores = jax.nn.sigmoid(share[rows, :])
            inverse = 1.0 / jnp.sum(scores, axis=1, keepdims=True)
            position = first + r0 + lax.broadcasted_iota(jnp.int32, (STRIP, 1), 0)
            valid = jnp.where(position < live, 1.0, 0.0)
            part = scores * inverse
            share[rows, :] = part
            part = part * valid
            coef[rows, :] = part * (1.0 - scores)
            score_sum = score_sum + part.reshape(STRIP // 8, 8, E).sum(axis=0)
        if c == 0:
            counts = ar_wait(0, 0)
            ar_send(0, 1, counts)
        if c == 2:
            counts = ar_wait(0, 1)
            ar_send(0, 2, counts)
    counts = ar_wait(0, 2)
    ar_send(1, 0, score_sum)

    tokens = live.astype(jnp.float32)
    fraction = E * counts[0:1] / (TOPK * tokens)
    weights = LOSS_SCALE * fraction / tokens
    for r0 in range(0, ROWS, 128):
        rows = pl.ds(r0, 128)
        weighted = jnp.sum(weights * share[rows, :], axis=1, keepdims=True)
        grad = (weights - weighted) * coef[rows, :]
        high = grad.astype(jnp.bfloat16)
        ghi[rows, :] = high
        glo[rows, :] = (grad - high.astype(jnp.float32)).astype(jnp.bfloat16)

    def d2d(j):
        return pltpu.make_async_remote_copy(
            src_ref=snd.at[j], dst_ref=got.at[j], send_sem=d2d_s.at[j], recv_sem=d2d_r.at[j],
            device_id=other, device_id_type=MESH,
        )

    def halving(s, k, where):
        return pltpu.make_async_remote_copy(
            src_ref=acc[s].at[where], dst_ref=rb[s].at[where], send_sem=cube_s.at[s, k], recv_sem=cube_r.at[s, k],
            device_id=cube[dimension(s, k)], device_id_type=MESH,
        )

    def upper(k):
        return (pl.ds(4 >> k, 4 >> k),)

    def straight(s, r):
        return pltpu.make_async_remote_copy(
            src_ref=acc[s].at[0, r], dst_ref=rb[s].at[0, r], send_sem=cube_s.at[s, 3], recv_sem=cube_r.at[s, 3],
            device_id=far[TURN[s] // 3][r], device_id_type=MESH,
        )

    def all_straight(s):
        return pltpu.make_async_remote_copy(
            src_ref=acc[s].at[0, pl.ds(1, 7)], dst_ref=rb[s].at[0, pl.ds(1, 7)], send_sem=cube_s.at[s, 3],
            recv_sem=cube_r.at[s, 3], device_id=far[TURN[s] // 3][1], device_id_type=MESH,
        )

    def final(i, where):
        return pltpu.make_async_remote_copy(
            src_ref=fin.at[(core, v) + where], dst_ref=fin.at[(core, v) + where], send_sem=fin_s.at[i],
            recv_sem=fin_r.at[i], device_id=(cube[5], cross, other)[i], device_id_type=MESH,
        )

    yhi, xhi = y // 2, x // 2
    ylo, xlo = (yhi + y) % 2, (xhi + x) % 2
    v = (zh + zlo) % 2

    def multiply(j):
        y_hi = (yhi + j // 4) % 2
        y_at = 2 * y_hi + (y_hi + ylo + (j // 2) % 2) % 2
        x_hi = (xhi + j) % 2
        start = (y_at * 2 + x_hi) * CHUNK
        for m in range(CHUNK // 128):
            part = h[:, pl.ds(pl.multiple_of(start + m * 128, 128), 128)]
            dims = (((0,), (0,)), ((), ()))
            made = lax.dot_general(part, ghi[...], dims, preferred_element_type=jnp.float32)
            made = made + lax.dot_general(part, glo[...], dims, preferred_element_type=jnp.float32)
            at = m * 128
            while at < (m + 1) * 128:
                to = min((at // HALF + 1) * HALF, (m + 1) * 128)
                piece = at // HALF
                b1 = (x_hi + piece // 4 + xlo) % 2
                b2 = (piece // 2 % 2 + zh) % 2
                b3 = (piece % 2 + v) % 2
                b = b1 * 4 + b2 * 2 + b3
                lo, size = at - piece * HALF, to - at
                own[j, b, lo : lo + size] = made[at - m * 128 : to - m * 128, :128]
                snd[j, b, lo : lo + size] = made[at - m * 128 : to - m * 128, 128:]
                at = to
        d2d(j).start()

    def gather(j):
        d2d(j).wait_recv()
        for b in range(8):
            total = own[j, b] + got[j, b]
            for s in range(NP):
                acc[s][place(s, j, b)] = total[OFFSET[s] : OFFSET[s] + 8 * TILES[s]]
        for s in range(NP):
            if TURN[s] >= 3:
                halving(s, 0, (pl.ds(4, 4), j)).start()
        for t, bit in ((0, j // 4), (1, (j // 2) % 2), (2, j % 2)):

            @pl.when(bit == 1)
            def _(t=t):
                for s in range(NP):
                    if TURN[s] == t:
                        halving(s, 0, (turn(j, t),)).start()

    def step(i, carry):
        @pl.when(i < 8)
        def _():
            multiply(7 - i)

        @pl.when(i > 0)
        def _():
            gather(8 - i)

        return carry

    lax.fori_loop(0, 9, step, 0)

    score_sum = ar_wait(1, 0)
    ar_send(1, 1, score_sum)

    for k in range(3):
        n = 4 >> k
        for s in range(NP):
            halving(s, k, upper(k)).wait_recv()
            acc[s][0:n] = acc[s][0:n] + rb[s][n : 2 * n]
            if k < 2:
                halving(s, k + 1, upper(k + 1)).start()
            else:
                for r in (7, 6, 5, 3, 4, 2, 1):
                    straight(s, r).start()
        if k == 1:
            score_sum = ar_wait(1, 1)
            ar_send(1, 2, score_sum)

    for half in range(2):
        for s in SET_OF[half]:
            all_straight(s).wait_recv()
            total = acc[s][0, 0]
            for r in range(1, 8):
                total = total + rb[s][0, r]
            fin[core, v, OFFSET[s] : OFFSET[s] + 8 * TILES[s]] = total
        for i in range(3):
            final(i, (pl.ds(*SET_ROWS[half]),)).start()

    score_sum = ar_wait(1, 2)
    mean_score = jnp.sum(score_sum, axis=0, keepdims=True) / tokens
    bal[0] = jnp.sum(fraction * mean_score)

    for s in range(NP):
        for k in range(3):
            halving(s, k, upper(k)).wait_send()
        all_straight(s).wait_send()
    for j in range(8):
        d2d(j).wait_send()
    for i in range(3):
        final(i, ()).wait()
    for e in range(2):
        for half in range(2):
            out[half * HALF : (half + 1) * HALF, e * 128 : (e + 1) * 128] = fin[e, half]


def solution(mesh):
    def shards(hidden, router_weight, expert_index, lengths):
        any_space = pl.BlockSpec(memory_space=pltpu.HBM)
        pieces = [(8, 8, 8 * t, 128) for t in TILES]
        return pl.pallas_call(
            kernel,
            out_shape=(jax.ShapeDtypeStruct((BLOCK, E), jnp.float32), jax.ShapeDtypeStruct((1,), jnp.float32)),
            in_specs=[any_space] * 4,
            out_specs=(pl.BlockSpec(memory_space=pltpu.VMEM), pl.BlockSpec(memory_space=pltpu.SMEM)),
            scratch_shapes=[
                pltpu.VMEM((ROWS, D), jnp.bfloat16),
                pltpu.VMEM((D, E), jnp.bfloat16),
                pltpu.VMEM((TOPK, ROWS), jnp.int32),
                pltpu.SMEM((1,), jnp.int32),
                pltpu.VMEM((ROWS, E), jnp.float32),
                pltpu.VMEM((ROWS, E), jnp.float32),
                pltpu.VMEM((ROWS, E), jnp.bfloat16),
                pltpu.VMEM((ROWS, E), jnp.bfloat16),
                pltpu.VMEM((8, 8, HALF, 128), jnp.float32),
                pltpu.VMEM((8, 8, HALF, 128), jnp.float32),
                pltpu.VMEM((8, 8, HALF, 128), jnp.float32),
                *[pltpu.VMEM(p, jnp.float32) for p in pieces],
                *[pltpu.VMEM(p, jnp.float32) for p in pieces],
                pltpu.VMEM((2, 2, HALF, 128), jnp.float32),
                pltpu.VMEM((2, 3, 4, 8, E), jnp.float32),
                pltpu.SemaphoreType.DMA((4 + HCH,)),
                pltpu.SemaphoreType.DMA((8,)),
                pltpu.SemaphoreType.DMA((8,)),
                pltpu.SemaphoreType.DMA((NP, 4)),
                pltpu.SemaphoreType.DMA((NP, 4)),
                pltpu.SemaphoreType.DMA((2, 3)),
                pltpu.SemaphoreType.DMA((2, 3)),
                pltpu.SemaphoreType.DMA((3,)),
                pltpu.SemaphoreType.DMA((3,)),
            ],
            compiler_params=pltpu.CompilerParams(
                collective_id=0, has_side_effects=True, vmem_limit_bytes=64487424
            ),
        )(hidden, router_weight, expert_index.T, lengths)

    return jax.shard_map(
        shards,
        mesh=mesh,
        in_specs=(P(("seq", "ctx"), None), P(), P(("seq", "ctx"), None), P("seq")),
        out_specs=(P("ctx", None), P("seq")),
        check_vma=False,
    )
```

```python
import jax
import jax.numpy as jnp
from jax import lax
from jax.experimental import pallas as pl
from jax.experimental.pallas import tpu as pltpu
from jax.sharding import PartitionSpec as P

D = 7168
E = 256
TOPK = 8
ROWS = 1024
BLOCK = 224
HALF = BLOCK // 2
CHUNK = 4 * BLOCK
LOSS_SCALE = 65536.0
MESH = pl.DeviceIdType.MESH

TILES = (3, 2, 2, 3, 2, 2)
OFFSET = tuple(8 * sum(TILES[:p]) for p in range(6))
FIRST, SECOND = (0, 1, 2), (3, 4, 5)
ROWS_OF = ((0, OFFSET[3]), (OFFSET[3], HALF - OFFSET[3]))

EVENTS = (
    (8, 0, 3), (8, 1, 3), (8, 2, 3), (9, 2, 2), (10, 0, 2), (11, 1, 2), (12, 1, 1), (12, 2, 1), (13, 0, 1),
    (16, 1, 0), (16, 2, 0), (17, 0, 0),
)
SOURCES = ((4, 2, 1), (5, 3), (6,), (7,))

HCH = 4
HROWS = ROWS // HCH
STRIP = 64


def turn(i, t):
    return (i, (i % 4) * 2 + i // 4, (i % 2) * 4 + i // 2)[t]


def place(p, j, b):
    return (turn(j, p), b) if p < 3 else (turn(b, p - 3), j)


def dimension(p, k):
    return (p + k) % 3 if p < 3 else 3 + (p + k) % 3


def kernel(hid, wt, eidx, lens, out, bal, *scratch):
    (h, w, idx, length, share, coef, ghi, glo, own, snd, got) = scratch[:11]
    acc, rb = scratch[11:17], scratch[17:23]
    (fin, ar, in_sem, d2d_s, d2d_r, one_s, one_r, two_s, two_r, far_s, far_r, ar_s, ar_r, fin_s, fin_r) = scratch[23:]

    seq, ctx = lax.axis_index("seq"), lax.axis_index("ctx")
    core, zlo = seq % 2, seq // 2
    zh, x, y = ctx % 2, (ctx // 2) % 4, ctx // 8

    def device(y_, x_, zh_, zlo_, core_):
        return (zlo_ * 2 + core_, (y_ * 4 + x_) * 2 + zh_)

    def across(bits):
        y_, x_, zh_, zlo_ = y, x, zh, zlo
        if bits & 32:
            y_ = 3 - y_
        if bits & 16:
            y_ = y_ + 1 - 2 * (y_ % 2)
        if bits & 8:
            x_ = 3 - x_
        if bits & 4:
            x_ = x_ + 1 - 2 * (x_ % 2)
        if bits & 2:
            zh_, zlo_ = 1 - zh_, 1 - zlo_
        if bits & 1:
            zlo_ = 1 - zlo_
        return device(y_, x_, zh_, zlo_, core)

    cube = [across(32 >> d) for d in range(6)]
    far = ([across(r) for r in range(8)], [across(8 * r) for r in range(8)])
    other = device(y, x, zh, zlo, 1 - core)
    cross = device(y, x, zh, 1 - zlo, 1 - core)
    ring_x = [device(y, (x + d) % 4, zh, zlo, core) for d in (1, 2, 3)]
    ring_y = [device((y + d) % 4, x, zh, zlo, core) for d in (1, 2, 3)]
    pair_z = [device(y, x, 1 - zh, zlo, core)]
    stages = ((ring_x, x), (ring_y, y), (pair_z, zh))

    barrier = pltpu.get_barrier_semaphore()
    greeted = [across(r) for r in range(1, 8)] + [across(8 * r) for r in range(1, 8)] + pair_z + [other, cross]
    greeted += [device(y, (x + 2) % 4, zh, zlo, core), device((y + 2) % 4, x, zh, zlo, core)]
    for peer in greeted:
        pl.semaphore_signal(barrier, inc=1, device_id=peer, device_id_type=MESH)

    load_len = pltpu.make_async_copy(lens, length, in_sem.at[0])
    load_idx = pltpu.make_async_copy(eidx, idx, in_sem.at[1])
    load_w = [
        pltpu.make_async_copy(
            wt.at[:, pl.ds(pl.multiple_of(((core + e) % 2) * 128, 128), 128)], w.at[:, e * 128 : (e + 1) * 128],
            in_sem.at[2 + e],
        )
        for e in range(2)
    ]
    load_h = [
        pltpu.make_async_copy(hid.at[pl.ds(c * HROWS, HROWS)], h.at[pl.ds(c * HROWS, HROWS)], in_sem.at[4 + c])
        for c in range(HCH)
    ]
    load_len.start()
    load_idx.start()
    for e in range(2):
        load_w[e].start()
    load_h[0].start()

    load_len.wait()
    load_idx.wait()
    live = length[0]
    start_at = ctx * ROWS

    hits = jnp.zeros((E, 128), jnp.float32)
    experts = (lax.broadcasted_iota(jnp.int32, (E, 128), 0) + core * 128) % E
    for i in range(ROWS // 128):
        block = idx[:, i * 128 : (i + 1) * 128]
        position = start_at + i * 128 + lax.broadcasted_iota(jnp.int32, block.shape, 1)
        block = jnp.where(position < live, block, -1)
        for k in range(TOPK):
            hits = hits + jnp.where(block[k : k + 1, :] == experts, 1.0, 0.0)
    counts = lax.dot_general(
        jnp.ones((8, 128), jnp.bfloat16), hits.astype(jnp.bfloat16), (((1,), (1,)), ((), ())),
        preferred_element_type=jnp.float32,
    )

    def ar_copy(kind, stage, peer, where):
        return pltpu.make_async_remote_copy(
            src_ref=ar.at[(kind, stage) + where],
            dst_ref=ar.at[(kind, stage) + where],
            send_sem=ar_s.at[kind, stage],
            recv_sem=ar_r.at[kind, stage],
            device_id=peer,
            device_id_type=MESH,
        )

    def ar_send(kind, stage, value):
        peers, mine = stages[stage]
        ar[kind, stage, mine] = value
        for peer in peers:
            ar_copy(kind, stage, peer, (mine,)).start()

    def ar_wait(kind, stage):
        peers, _ = stages[stage]
        n = len(peers)
        ar_copy(kind, stage, peers[0], (pl.ds(0, n),)).wait()
        total = ar[kind, stage, 0]
        for i in range(1, n + 1):
            total = total + ar[kind, stage, i]
        return total

    load_h[1].start()
    pl.semaphore_wait(barrier, len(greeted))
    ar_send(0, 0, counts)

    for e in range(2):
        load_w[e].wait()
    score_sum = jnp.zeros((8, E), jnp.float32)
    for c in range(HCH):
        rows = pl.ds(c * HROWS, HROWS)
        load_h[c].wait()
        if c + 2 < HCH:
            load_h[c + 2].start()
        share[rows, :] = jnp.dot(h[rows, :], w[...], preferred_element_type=jnp.float32)
        for r0 in range(c * HROWS, (c + 1) * HROWS, STRIP):
            rows = pl.ds(r0, STRIP)
            scores = jax.nn.sigmoid(share[rows, :])
            inverse = 1.0 / jnp.sum(scores, axis=1, keepdims=True)
            position = start_at + r0 + lax.broadcasted_iota(jnp.int32, (STRIP, 1), 0)
            valid = jnp.where(position < live, 1.0, 0.0)
            part = scores * inverse
            share[rows, :] = part
            part = part * valid
            coef[rows, :] = part * (1.0 - scores)
            score_sum = score_sum + part.reshape(STRIP // 8, 8, E).sum(axis=0)
        if c == 0:
            counts = ar_wait(0, 0)
            ar_send(0, 1, counts)
        if c == 2:
            counts = ar_wait(0, 1)
            ar_send(0, 2, counts)
    counts = ar_wait(0, 2)
    ar_send(1, 0, score_sum)

    tokens = live.astype(jnp.float32)
    fraction = E * counts[0:1] / (TOPK * tokens)
    weights = LOSS_SCALE * fraction / tokens
    for r0 in range(0, ROWS, 128):
        rows = pl.ds(r0, 128)
        weighted = jnp.sum(weights * share[rows, :], axis=1, keepdims=True)
        grad = (weights - weighted) * coef[rows, :]
        high = grad.astype(jnp.bfloat16)
        ghi[rows, :] = high
        glo[rows, :] = (grad - high.astype(jnp.float32)).astype(jnp.bfloat16)

    def d2d(j):
        return pltpu.make_async_remote_copy(
            src_ref=snd.at[j], dst_ref=got.at[j], send_sem=d2d_s.at[j], recv_sem=d2d_r.at[j],
            device_id=other, device_id_type=MESH,
        )

    def first(p, k, r):
        return pltpu.make_async_remote_copy(
            src_ref=acc[p].at[r], dst_ref=rb[p].at[r], send_sem=one_s.at[p, r], recv_sem=one_r.at[p, r],
            device_id=cube[dimension(p, k)], device_id_type=MESH,
        )

    def second(p, k, j):
        where = (pl.ds(4 >> k, 4 >> k), j)
        return pltpu.make_async_remote_copy(
            src_ref=acc[p].at[where], dst_ref=rb[p].at[where], send_sem=two_s.at[p - 3, k, j],
            recv_sem=two_r.at[p - 3, k, j], device_id=cube[dimension(p, k)], device_id_type=MESH,
        )

    def straight(p, r):
        return pltpu.make_async_remote_copy(
            src_ref=acc[p].at[0, r], dst_ref=rb[p].at[0, r], send_sem=far_s.at[p], recv_sem=far_r.at[p],
            device_id=far[p // 3][r], device_id_type=MESH,
        )

    def all_straight(p):
        where = (0, pl.ds(1, 7))
        return pltpu.make_async_remote_copy(
            src_ref=acc[p].at[where], dst_ref=rb[p].at[where], send_sem=far_s.at[p], recv_sem=far_r.at[p],
            device_id=far[p // 3][1], device_id_type=MESH,
        )

    def final(i, where):
        return pltpu.make_async_remote_copy(
            src_ref=fin.at[(core, v) + where], dst_ref=fin.at[(core, v) + where], send_sem=fin_s.at[i],
            recv_sem=fin_r.at[i], device_id=(cube[5], cross, other)[i], device_id_type=MESH,
        )

    yhi, xhi = y // 2, x // 2
    ylo, xlo = (yhi + y) % 2, (xhi + x) % 2
    v = (zh + zlo) % 2

    def multiply(j):
        y_hi = (yhi + j // 4) % 2
        y_at = 2 * y_hi + (y_hi + ylo + (j // 2) % 2) % 2
        x_hi = (xhi + j) % 2
        start = (y_at * 2 + x_hi) * CHUNK
        for m in range(CHUNK // 128):
            part = h[:, pl.ds(pl.multiple_of(start + m * 128, 128), 128)]
            dims = (((0,), (0,)), ((), ()))
            made = lax.dot_general(part, ghi[...], dims, preferred_element_type=jnp.float32)
            made = made + lax.dot_general(part, glo[...], dims, preferred_element_type=jnp.float32)
            at = m * 128
            while at < (m + 1) * 128:
                to = min((at // HALF + 1) * HALF, (m + 1) * 128)
                piece = at // HALF
                b1 = (x_hi + piece // 4 + xlo) % 2
                b2 = (piece // 2 % 2 + zh) % 2
                b3 = (piece % 2 + v) % 2
                b = b1 * 4 + b2 * 2 + b3
                lo, size = at - piece * HALF, to - at
                own[j, b, lo : lo + size] = made[at - m * 128 : to - m * 128, :128]
                snd[j, b, lo : lo + size] = made[at - m * 128 : to - m * 128, 128:]
                at = to
        d2d(j).start()

    def gather(j):
        d2d(j).wait_recv()
        for b in range(8):
            total = own[j, b] + got[j, b]
            for s in range(6):
                acc[s][place(s, j, b)] = total[OFFSET[s] : OFFSET[s] + 8 * TILES[s]]
        for p in SECOND:
            second(p, 0, j).start()
        for p, bit in ((0, j // 4), (1, (j // 2) % 2), (2, j % 2)):

            @pl.when(bit == 1)
            def _(p=p):
                first(p, 0, turn(j, p)).start()

    def advance(p, r):
        total = acc[p][r]
        for source in SOURCES[r]:
            first(p, 0 if source >= 4 else 1 if source >= 2 else 2, source).wait_recv()
            total = total + rb[p][source]
        acc[p][r] = total
        if r > 0:
            first(p, 1 if r >= 2 else 2, r).start()
        else:
            for b in (7, 6, 5, 3, 4, 2, 1):
                straight(p, b).start()

    def step(i, carry):
        @pl.when(i < 8)
        def _():
            multiply(7 - i)

        @pl.when((i > 1) & (i < 10))
        def _():
            gather(9 - i)

        @pl.when(i == 5)
        def _():
            ar_send(1, 1, ar_wait(1, 0))

        for at in sorted({at for at, _, _ in EVENTS}):

            @pl.when(i == at)
            def _(at=at):
                for at_, p, r in EVENTS:
                    if at_ == at:
                        advance(p, r)

        @pl.when((i > 5) & (i < 14))
        def _():
            j = 13 - i
            for p in SECOND:
                second(p, 0, j).wait_recv()
                acc[p][0:4, j] = acc[p][0:4, j] + rb[p][4:8, j]
                second(p, 1, j).start()

        @pl.when((i > 8) & (i < 17))
        def _():
            j = 16 - i
            for p in SECOND:
                second(p, 1, j).wait_recv()
                acc[p][0:2, j] = acc[p][0:2, j] + rb[p][2:4, j]
                second(p, 2, j).start()

        @pl.when(i == 10)
        def _():
            ar_send(1, 2, ar_wait(1, 1))

        @pl.when(i > 11)
        def _():
            j = 19 - i
            for p in SECOND:
                second(p, 2, j).wait_recv()
                acc[p][0, j] = acc[p][0, j] + rb[p][1, j]

        for r in range(1, 8):

            @pl.when(i == 19 - r)
            def _(r=r):
                for p in SECOND:
                    straight(p, r).start()

        return carry

    lax.fori_loop(0, 20, step, 0)

    for half, pieces in enumerate((FIRST, SECOND)):
        for p in pieces:
            all_straight(p).wait_recv()
            total = acc[p][0, 0]
            for r in range(1, 8):
                total = total + rb[p][0, r]
            fin[core, v, OFFSET[p] : OFFSET[p] + 8 * TILES[p]] = total
        for i in range(3):
            final(i, (pl.ds(*ROWS_OF[half]),)).start()

    score_sum = ar_wait(1, 2)
    mean_score = jnp.sum(score_sum, axis=0, keepdims=True) / tokens
    bal[0] = jnp.sum(fraction * mean_score)

    for p in FIRST:
        for r in range(1, 8):
            first(p, 0, r).wait_send()
    for p in SECOND:
        for k in range(3):
            for j in range(8):
                second(p, k, j).wait_send()
    for p in range(6):
        all_straight(p).wait_send()
    for j in range(8):
        d2d(j).wait_send()
    for i in range(3):
        final(i, ()).wait()
    for e in range(2):
        for half in range(2):
            out[half * HALF : (half + 1) * HALF, e * 128 : (e + 1) * 128] = fin[e, half]


def solution(mesh):
    def shards(hidden, router_weight, expert_index, lengths):
        any_space = pl.BlockSpec(memory_space=pltpu.HBM)
        pieces = [(8, 8, 8 * t, 128) for t in TILES]
        return pl.pallas_call(
            kernel,
            out_shape=(pltpu.VMEM((BLOCK, E), jnp.float32), jax.ShapeDtypeStruct((1,), jnp.float32)),
            in_specs=[any_space] * 4,
            out_specs=(pl.BlockSpec(memory_space=pltpu.VMEM), pl.BlockSpec(memory_space=pltpu.SMEM)),
            scratch_shapes=[
                pltpu.VMEM((ROWS, D), jnp.bfloat16),
                pltpu.VMEM((D, E), jnp.bfloat16),
                pltpu.VMEM((TOPK, ROWS), jnp.int32),
                pltpu.SMEM((1,), jnp.int32),
                pltpu.VMEM((ROWS, E), jnp.float32),
                pltpu.VMEM((ROWS, E), jnp.float32),
                pltpu.VMEM((ROWS, E), jnp.bfloat16),
                pltpu.VMEM((ROWS, E), jnp.bfloat16),
                pltpu.VMEM((8, 8, HALF, 128), jnp.float32),
                pltpu.VMEM((8, 8, HALF, 128), jnp.float32),
                pltpu.VMEM((8, 8, HALF, 128), jnp.float32),
                *[pltpu.VMEM(p, jnp.float32) for p in pieces],
                *[pltpu.VMEM(p, jnp.float32) for p in pieces],
                pltpu.VMEM((2, 2, HALF, 128), jnp.float32),
                pltpu.VMEM((2, 3, 4, 8, E), jnp.float32),
                pltpu.SemaphoreType.DMA((4 + HCH,)),
                pltpu.SemaphoreType.DMA((8,)),
                pltpu.SemaphoreType.DMA((8,)),
                pltpu.SemaphoreType.DMA((3, 8)),
                pltpu.SemaphoreType.DMA((3, 8)),
                pltpu.SemaphoreType.DMA((3, 3, 8)),
                pltpu.SemaphoreType.DMA((3, 3, 8)),
                pltpu.SemaphoreType.DMA((6,)),
                pltpu.SemaphoreType.DMA((6,)),
                pltpu.SemaphoreType.DMA((2, 3)),
                pltpu.SemaphoreType.DMA((2, 3)),
                pltpu.SemaphoreType.DMA((3,)),
                pltpu.SemaphoreType.DMA((3,)),
            ],
            compiler_params=pltpu.CompilerParams(
                collective_id=0, has_side_effects=True, vmem_limit_bytes=64487424
            ),
        )(hidden, router_weight, expert_index.T, lengths)

    return jax.shard_map(
        shards,
        mesh=mesh,
        in_specs=(P(("seq", "ctx"), None), P(), P(("seq", "ctx"), None), P("seq")),
        out_specs=(P("ctx", None), P("seq")),
        check_vma=False,
    )
```

```python
import jax
import jax.numpy as jnp
from jax import lax
from jax.experimental import pallas as pl
from jax.experimental.pallas import tpu as pltpu
from jax.sharding import PartitionSpec as P

D = 7168
E = 256
TOPK = 8
ROWS = 1024
BLOCK = 224
HALF = BLOCK // 2
CHUNK = 4 * BLOCK
LOSS_SCALE = 65536.0
MESH = pl.DeviceIdType.MESH

TILES = (3, 2, 2, 3, 2, 2)
OFFSET = tuple(8 * sum(TILES[:p]) for p in range(6))
FIRST, SECOND = (0, 1, 2), (3, 4, 5)
ROWS_OF = ((0, OFFSET[3]), (OFFSET[3], HALF - OFFSET[3]))

EVENTS = (
    (6, 1, 3), (7, 2, 3), (8, 0, 3), (8, 2, 2), (10, 0, 2), (10, 1, 2), (11, 1, 1), (11, 2, 1), (12, 0, 1),
    (14, 1, 0), (14, 2, 0), (15, 0, 0),
)
SOURCES = ((4, 2, 1), (5, 3), (6,), (7,))

HCH = 4
HROWS = ROWS // HCH
STRIP = 64


def turn(i, t):
    return (i, (i % 4) * 2 + i // 4, (i % 2) * 4 + i // 2)[t]


def place(p, j, b):
    return (turn(j, p), b) if p < 3 else (turn(b, p - 3), j)


def dimension(p, k):
    return (p + k) % 3 if p < 3 else 3 + (p + k) % 3


def kernel(hid, wt, eidx, lens, out, bal, *scratch):
    (h, w, idx, length, share, coef, ghi, glo, own, snd, got) = scratch[:11]
    acc, rb = scratch[11:17], scratch[17:23]
    (fin, ar, in_sem, d2d_s, d2d_r, one_s, one_r, two_s, two_r, far_s, far_r, ar_s, ar_r, fin_s, fin_r) = scratch[23:]

    seq, ctx = lax.axis_index("seq"), lax.axis_index("ctx")
    core, zlo = seq % 2, seq // 2
    zh, x, y = ctx % 2, (ctx // 2) % 4, ctx // 8

    def device(y_, x_, zh_, zlo_, core_):
        return (zlo_ * 2 + core_, (y_ * 4 + x_) * 2 + zh_)

    def across(bits):
        y_, x_, zh_, zlo_ = y, x, zh, zlo
        if bits & 32:
            y_ = 3 - y_
        if bits & 16:
            y_ = y_ + 1 - 2 * (y_ % 2)
        if bits & 8:
            x_ = 3 - x_
        if bits & 4:
            x_ = x_ + 1 - 2 * (x_ % 2)
        if bits & 2:
            zh_, zlo_ = 1 - zh_, 1 - zlo_
        if bits & 1:
            zlo_ = 1 - zlo_
        return device(y_, x_, zh_, zlo_, core)

    cube = [across(32 >> d) for d in range(6)]
    far = ([across(r) for r in range(8)], [across(8 * r) for r in range(8)])
    other = device(y, x, zh, zlo, 1 - core)
    cross = device(y, x, zh, 1 - zlo, 1 - core)
    plane = [device(y, (x + d // 2) % 4, (zh + d) % 2, zlo, core) for d in range(1, 8)]
    ring_y = [device((y + d) % 4, x, zh, zlo, core) for d in (1, 2, 3)]
    stages = ((plane, x * 2 + zh), (ring_y, y))

    barrier = pltpu.get_barrier_semaphore()
    greeted = plane + ring_y + [across(r) for r in (1, 2, 3, 5, 6, 7)] + [across(8 * r) for r in (3, 5, 6, 7)]
    greeted += [other, cross]
    for peer in greeted:
        pl.semaphore_signal(barrier, inc=1, device_id=peer, device_id_type=MESH)

    load_len = pltpu.make_async_copy(lens, length, in_sem.at[0])
    load_idx = pltpu.make_async_copy(eidx, idx, in_sem.at[1])
    load_w = [
        pltpu.make_async_copy(
            wt.at[:, pl.ds(pl.multiple_of(((core + e) % 2) * 128, 128), 128)], w.at[:, e * 128 : (e + 1) * 128],
            in_sem.at[2 + e],
        )
        for e in range(2)
    ]
    load_h = [
        pltpu.make_async_copy(hid.at[pl.ds(c * HROWS, HROWS)], h.at[pl.ds(c * HROWS, HROWS)], in_sem.at[4 + c])
        for c in range(HCH)
    ]
    load_len.start()
    load_idx.start()
    for e in range(2):
        load_w[e].start()
    load_h[0].start()

    load_len.wait()
    load_idx.wait()
    live = length[0]
    start_at = ctx * ROWS

    hits = jnp.zeros((E, 128), jnp.float32)
    experts = (lax.broadcasted_iota(jnp.int32, (E, 128), 0) + core * 128) % E
    for i in range(ROWS // 128):
        block = idx[:, i * 128 : (i + 1) * 128]
        position = start_at + i * 128 + lax.broadcasted_iota(jnp.int32, block.shape, 1)
        block = jnp.where(position < live, block, -1)
        for k in range(TOPK):
            hits = hits + jnp.where(block[k : k + 1, :] == experts, 1.0, 0.0)
    counts = lax.dot_general(
        jnp.ones((8, 128), jnp.bfloat16), hits.astype(jnp.bfloat16), (((1,), (1,)), ((), ())),
        preferred_element_type=jnp.float32,
    )

    def ar_copy(kind, stage, peer, where):
        return pltpu.make_async_remote_copy(
            src_ref=ar.at[(kind, stage) + where],
            dst_ref=ar.at[(kind, stage) + where],
            send_sem=ar_s.at[kind, stage],
            recv_sem=ar_r.at[kind, stage],
            device_id=peer,
            device_id_type=MESH,
        )

    def ar_send(kind, stage, value):
        peers, mine = stages[stage]
        ar[kind, stage, mine] = value
        for peer in peers:
            ar_copy(kind, stage, peer, (mine,)).start()

    def ar_wait(kind, stage):
        peers, _ = stages[stage]
        n = len(peers)
        ar_copy(kind, stage, peers[0], (pl.ds(0, n),)).wait()
        total = ar[kind, stage, 0]
        for i in range(1, n + 1):
            total = total + ar[kind, stage, i]
        return total

    load_h[1].start()
    pl.semaphore_wait(barrier, len(greeted))
    ar_send(0, 0, counts[0:1])

    for e in range(2):
        load_w[e].wait()
    score_sum = jnp.zeros((8, E), jnp.float32)
    for c in range(HCH):
        rows = pl.ds(c * HROWS, HROWS)
        load_h[c].wait()
        if c + 2 < HCH:
            load_h[c + 2].start()
        share[rows, :] = jnp.dot(h[rows, :], w[...], preferred_element_type=jnp.float32)
        for r0 in range(c * HROWS, (c + 1) * HROWS, STRIP):
            rows = pl.ds(r0, STRIP)
            scores = jax.nn.sigmoid(share[rows, :])
            inverse = 1.0 / jnp.sum(scores, axis=1, keepdims=True)
            position = start_at + r0 + lax.broadcasted_iota(jnp.int32, (STRIP, 1), 0)
            valid = jnp.where(position < live, 1.0, 0.0)
            part = scores * inverse
            share[rows, :] = part
            part = part * valid
            coef[rows, :] = part * (1.0 - scores)
            score_sum = score_sum + part.reshape(STRIP // 8, 8, E).sum(axis=0)
        if c == 1:
            counts = ar_wait(0, 0)
            ar_send(0, 1, counts)
    counts = ar_wait(0, 1)
    ar_send(1, 0, jnp.sum(score_sum, axis=0, keepdims=True))

    tokens = live.astype(jnp.float32)
    fraction = E * counts / (TOPK * tokens)
    weights = LOSS_SCALE * fraction / tokens
    for r0 in range(0, ROWS, 128):
        rows = pl.ds(r0, 128)
        weighted = jnp.sum(weights * share[rows, :], axis=1, keepdims=True)
        grad = (weights - weighted) * coef[rows, :]
        high = grad.astype(jnp.bfloat16)
        ghi[rows, :] = high
        glo[rows, :] = (grad - high.astype(jnp.float32)).astype(jnp.bfloat16)

    def d2d(j):
        return pltpu.make_async_remote_copy(
            src_ref=snd.at[j], dst_ref=got.at[j], send_sem=d2d_s.at[j], recv_sem=d2d_r.at[j],
            device_id=other, device_id_type=MESH,
        )

    def first(p, k, r):
        return pltpu.make_async_remote_copy(
            src_ref=acc[p].at[r], dst_ref=rb[p].at[r], send_sem=one_s.at[p, r], recv_sem=one_r.at[p, r],
            device_id=cube[dimension(p, k)], device_id_type=MESH,
        )

    def second(p, k, j):
        where = (pl.ds(4 >> k, 4 >> k), j)
        return pltpu.make_async_remote_copy(
            src_ref=acc[p].at[where], dst_ref=rb[p].at[where], send_sem=two_s.at[p - 3, k, j],
            recv_sem=two_r.at[p - 3, k, j], device_id=cube[dimension(p, k)], device_id_type=MESH,
        )

    def straight(p, r):
        return pltpu.make_async_remote_copy(
            src_ref=acc[p].at[0, r], dst_ref=rb[p].at[0, r], send_sem=far_s.at[p], recv_sem=far_r.at[p],
            device_id=far[p // 3][r], device_id_type=MESH,
        )

    def all_straight(p):
        where = (0, pl.ds(1, 7))
        return pltpu.make_async_remote_copy(
            src_ref=acc[p].at[where], dst_ref=rb[p].at[where], send_sem=far_s.at[p], recv_sem=far_r.at[p],
            device_id=far[p // 3][1], device_id_type=MESH,
        )

    def final(i, where):
        return pltpu.make_async_remote_copy(
            src_ref=fin.at[(core, v) + where], dst_ref=fin.at[(core, v) + where], send_sem=fin_s.at[i],
            recv_sem=fin_r.at[i], device_id=(cube[5], cross, other)[i], device_id_type=MESH,
        )

    yhi, xhi = y // 2, x // 2
    ylo, xlo = (yhi + y) % 2, (xhi + x) % 2
    v = (zh + zlo) % 2

    def multiply(j):
        y_hi = (yhi + j // 4) % 2
        y_at = 2 * y_hi + (y_hi + ylo + (j // 2) % 2) % 2
        x_hi = (xhi + j) % 2
        start = (y_at * 2 + x_hi) * CHUNK
        for m in range(CHUNK // 128):
            part = h[:, pl.ds(pl.multiple_of(start + m * 128, 128), 128)]
            dims = (((0,), (0,)), ((), ()))
            made = lax.dot_general(part, ghi[...], dims, preferred_element_type=jnp.float32)
            made = made + lax.dot_general(part, glo[...], dims, preferred_element_type=jnp.float32)
            at = m * 128
            while at < (m + 1) * 128:
                to = min((at // HALF + 1) * HALF, (m + 1) * 128)
                piece = at // HALF
                b1 = (x_hi + piece // 4 + xlo) % 2
                b2 = (piece // 2 % 2 + zh) % 2
                b3 = (piece % 2 + v) % 2
                b = b1 * 4 + b2 * 2 + b3
                lo, size = at - piece * HALF, to - at
                own[j, b, lo : lo + size] = made[at - m * 128 : to - m * 128, :128]
                snd[j, b, lo : lo + size] = made[at - m * 128 : to - m * 128, 128:]
                at = to
        d2d(j).start()

    def gather(j):
        d2d(j).wait_recv()
        for b in range(8):
            total = own[j, b] + got[j, b]
            for s in range(6):
                acc[s][place(s, j, b)] = total[OFFSET[s] : OFFSET[s] + 8 * TILES[s]]
        for p in SECOND:
            second(p, 0, j).start()
        for p, bit in ((0, j // 4), (1, (j // 2) % 2), (2, j % 2)):

            @pl.when(bit == 1)
            def _(p=p):
                first(p, 0, turn(j, p)).start()

    def advance(p, r):
        total = acc[p][r]
        for source in SOURCES[r]:
            first(p, 0 if source >= 4 else 1 if source >= 2 else 2, source).wait_recv()
            total = total + rb[p][source]
        acc[p][r] = total
        if r > 0:
            first(p, 1 if r >= 2 else 2, r).start()
        else:
            for b in (7, 6, 5, 3, 4, 2, 1):
                straight(p, b).start()

    def step(i, carry):
        @pl.when(i < 8)
        def _():
            multiply(7 - i)

        @pl.when((i > 1) & (i < 10))
        def _():
            gather(9 - i)

        @pl.when(i == 7)
        def _():
            ar_send(1, 1, ar_wait(1, 0))

        for at in sorted({at for at, _, _ in EVENTS}):

            @pl.when(i == at)
            def _(at=at):
                for at_, p, r in EVENTS:
                    if at_ == at:
                        advance(p, r)

        @pl.when((i > 4) & (i < 13))
        def _():
            j = 12 - i
            for p in SECOND:
                second(p, 0, j).wait_recv()
                acc[p][0:4, j] = acc[p][0:4, j] + rb[p][4:8, j]
                second(p, 1, j).start()

        @pl.when((i > 7) & (i < 16))
        def _():
            j = 15 - i
            for p in SECOND:
                second(p, 1, j).wait_recv()
                acc[p][0:2, j] = acc[p][0:2, j] + rb[p][2:4, j]
                second(p, 2, j).start()

        @pl.when((i > 10) & (i < 19))
        def _():
            j = 18 - i
            for p in SECOND:
                second(p, 2, j).wait_recv()
                acc[p][0, j] = acc[p][0, j] + rb[p][1, j]

        for r in range(1, 8):

            @pl.when(i == 18 - r)
            def _(r=r):
                for p in SECOND:
                    straight(p, r).start()

        return carry

    lax.fori_loop(0, 19, step, 0)

    for half, pieces in enumerate((FIRST, SECOND)):
        for p in pieces:
            all_straight(p).wait_recv()
            total = acc[p][0, 0]
            for r in range(1, 8):
                total = total + rb[p][0, r]
            fin[core, v, OFFSET[p] : OFFSET[p] + 8 * TILES[p]] = total
        for i in range(3):
            final(i, (pl.ds(*ROWS_OF[half]),)).start()

    score_sum = ar_wait(1, 1)
    mean_score = score_sum / tokens
    bal[0] = jnp.sum(fraction * mean_score)

    for p in FIRST:
        for r in range(1, 8):
            first(p, 0, r).wait_send()
    for p in SECOND:
        for k in range(3):
            for j in range(8):
                second(p, k, j).wait_send()
    for p in range(6):
        all_straight(p).wait_send()
    for j in range(8):
        d2d(j).wait_send()
    for i in range(3):
        final(i, ()).wait()
    for e in range(2):
        for half in range(2):
            out[half * HALF : (half + 1) * HALF, e * 128 : (e + 1) * 128] = fin[e, half]


def solution(mesh):
    def shards(hidden, router_weight, expert_index, lengths):
        any_space = pl.BlockSpec(memory_space=pltpu.HBM)
        pieces = [(8, 8, 8 * t, 128) for t in TILES]
        return pl.pallas_call(
            kernel,
            out_shape=(pltpu.VMEM((BLOCK, E), jnp.float32), jax.ShapeDtypeStruct((1,), jnp.float32)),
            in_specs=[any_space] * 4,
            out_specs=(pl.BlockSpec(memory_space=pltpu.VMEM), pl.BlockSpec(memory_space=pltpu.SMEM)),
            scratch_shapes=[
                pltpu.VMEM((ROWS, D), jnp.bfloat16),
                pltpu.VMEM((D, E), jnp.bfloat16),
                pltpu.VMEM((TOPK, ROWS), jnp.int32),
                pltpu.SMEM((1,), jnp.int32),
                pltpu.VMEM((ROWS, E), jnp.float32),
                pltpu.VMEM((ROWS, E), jnp.float32),
                pltpu.VMEM((ROWS, E), jnp.bfloat16),
                pltpu.VMEM((ROWS, E), jnp.bfloat16),
                pltpu.VMEM((8, 8, HALF, 128), jnp.float32),
                pltpu.VMEM((8, 8, HALF, 128), jnp.float32),
                pltpu.VMEM((8, 8, HALF, 128), jnp.float32),
                *[pltpu.VMEM(p, jnp.float32) for p in pieces],
                *[pltpu.VMEM(p, jnp.float32) for p in pieces],
                pltpu.VMEM((2, 2, HALF, 128), jnp.float32),
                pltpu.VMEM((2, 2, 8, 1, E), jnp.float32),
                pltpu.SemaphoreType.DMA((4 + HCH,)),
                pltpu.SemaphoreType.DMA((8,)),
                pltpu.SemaphoreType.DMA((8,)),
                pltpu.SemaphoreType.DMA((3, 8)),
                pltpu.SemaphoreType.DMA((3, 8)),
                pltpu.SemaphoreType.DMA((3, 3, 8)),
                pltpu.SemaphoreType.DMA((3, 3, 8)),
                pltpu.SemaphoreType.DMA((6,)),
                pltpu.SemaphoreType.DMA((6,)),
                pltpu.SemaphoreType.DMA((2, 2)),
                pltpu.SemaphoreType.DMA((2, 2)),
                pltpu.SemaphoreType.DMA((3,)),
                pltpu.SemaphoreType.DMA((3,)),
            ],
            compiler_params=pltpu.CompilerParams(
                collective_id=0, has_side_effects=True, vmem_limit_bytes=64487424
            ),
        )(hidden, router_weight, expert_index.T, lengths)

    return jax.shard_map(
        shards,
        mesh=mesh,
        in_specs=(P(("seq", "ctx"), None), P(), P(("seq", "ctx"), None), P("seq")),
        out_specs=(P("ctx", None), P("seq")),
        check_vma=False,
    )
```

```python
import jax
import jax.numpy as jnp
from jax import lax
from jax.experimental import pallas as pl
from jax.experimental.pallas import tpu as pltpu
from jax.sharding import PartitionSpec as P

D = 7168
E = 256
TOPK = 8
ROWS = 1024
BLOCK = 224
HALF = BLOCK // 2
CHUNK = 4 * BLOCK
LOSS_SCALE = 65536.0
MESH = pl.DeviceIdType.MESH

TILES = (3, 2, 2, 3, 2, 2)
OFFSET = tuple(8 * sum(TILES[:p]) for p in range(6))
FIRST, SECOND = (0, 1, 2), (3, 4, 5)
ROWS_OF = ((0, OFFSET[3]), (OFFSET[3], HALF - OFFSET[3]))

EVENTS = (
    (6, 1, 3), (7, 2, 3), (8, 0, 3), (8, 2, 2), (10, 0, 2), (10, 1, 2), (11, 1, 1), (11, 2, 1), (12, 0, 1),
    (14, 1, 0), (14, 2, 0), (15, 0, 0),
)
SOURCES = ((4, 2, 1), (5, 3), (6,), (7,))

HCH = 4
HROWS = ROWS // HCH
STRIP = 64


def turn(i, t):
    return (i, (i % 4) * 2 + i // 4, (i % 2) * 4 + i // 2)[t]


def place(p, j, b):
    return (turn(j, p), b) if p < 3 else (turn(b, p - 3), j)


def dimension(p, k):
    return (p + k) % 3 if p < 3 else 3 + (p + k) % 3


def kernel(hid, wt, eidx, lens, out, bal, *scratch):
    (h, w, idx, length, share, coef, ghi, glo, own, snd, got) = scratch[:11]
    acc, rb = scratch[11:17], scratch[17:23]
    (fin, ar, in_sem, d2d_s, d2d_r, one_s, one_r, two_s, two_r, far_s, far_r, ar_s, ar_r, fin_s, fin_r) = scratch[23:]

    seq, ctx = lax.axis_index("seq"), lax.axis_index("ctx")
    core, zlo = seq % 2, seq // 2
    zh, x, y = ctx % 2, (ctx // 2) % 4, ctx // 8

    def device(y_, x_, zh_, zlo_, core_):
        return (zlo_ * 2 + core_, (y_ * 4 + x_) * 2 + zh_)

    def across(bits):
        y_, x_, zh_, zlo_ = y, x, zh, zlo
        if bits & 32:
            y_ = 3 - y_
        if bits & 16:
            y_ = y_ + 1 - 2 * (y_ % 2)
        if bits & 8:
            x_ = 3 - x_
        if bits & 4:
            x_ = x_ + 1 - 2 * (x_ % 2)
        if bits & 2:
            zh_, zlo_ = 1 - zh_, 1 - zlo_
        if bits & 1:
            zlo_ = 1 - zlo_
        return device(y_, x_, zh_, zlo_, core)

    cube = [across(32 >> d) for d in range(6)]
    far = ([across(r) for r in range(8)], [across(8 * r) for r in range(8)])
    other = device(y, x, zh, zlo, 1 - core)
    cross = device(y, x, zh, 1 - zlo, 1 - core)
    plane = [device(y, (x + d // 2) % 4, (zh + d) % 2, zlo, core) for d in range(1, 8)]
    ring_y = [device((y + d) % 4, x, zh, zlo, core) for d in (1, 2, 3)]
    stages = ((plane, x * 2 + zh), (ring_y, y))

    barrier = pltpu.get_barrier_semaphore()
    greeted = plane + ring_y + [across(r) for r in (1, 2, 3, 5, 6, 7)] + [across(8 * r) for r in (3, 5, 6, 7)]
    greeted += [other, cross]
    for peer in greeted:
        pl.semaphore_signal(barrier, inc=1, device_id=peer, device_id_type=MESH)

    load_len = pltpu.make_async_copy(lens, length, in_sem.at[0])
    load_idx = pltpu.make_async_copy(eidx, idx, in_sem.at[1])
    load_w = [
        pltpu.make_async_copy(
            wt.at[:, pl.ds(pl.multiple_of(((core + e) % 2) * 128, 128), 128)], w.at[:, e * 128 : (e + 1) * 128],
            in_sem.at[2 + e],
        )
        for e in range(2)
    ]
    load_h = [
        pltpu.make_async_copy(hid.at[pl.ds(c * HROWS, HROWS)], h.at[pl.ds(c * HROWS, HROWS)], in_sem.at[4 + c])
        for c in range(HCH)
    ]
    load_len.start()
    load_idx.start()
    for e in range(2):
        load_w[e].start()
    load_h[0].start()

    load_len.wait()
    load_idx.wait()
    live = length[0]
    start_at = ctx * ROWS

    hits = jnp.zeros((E, 128), jnp.float32)
    experts = (lax.broadcasted_iota(jnp.int32, (E, 128), 0) + core * 128) % E
    for i in range(ROWS // 128):
        block = idx[:, i * 128 : (i + 1) * 128]
        position = start_at + i * 128 + lax.broadcasted_iota(jnp.int32, block.shape, 1)
        block = jnp.where(position < live, block, -1)
        for k in range(TOPK):
            hits = hits + jnp.where(block[k : k + 1, :] == experts, 1.0, 0.0)
    counts = lax.dot_general(
        jnp.ones((8, 128), jnp.bfloat16), hits.astype(jnp.bfloat16), (((1,), (1,)), ((), ())),
        preferred_element_type=jnp.float32,
    )

    def ar_copy(kind, stage, peer, where):
        return pltpu.make_async_remote_copy(
            src_ref=ar.at[(kind, stage) + where],
            dst_ref=ar.at[(kind, stage) + where],
            send_sem=ar_s.at[kind, stage],
            recv_sem=ar_r.at[kind, stage],
            device_id=peer,
            device_id_type=MESH,
        )

    def ar_send(kind, stage, value):
        peers, mine = stages[stage]
        ar[kind, stage, mine] = value
        for peer in peers:
            ar_copy(kind, stage, peer, (mine,)).start()

    def ar_wait(kind, stage):
        peers, _ = stages[stage]
        n = len(peers)
        ar_copy(kind, stage, peers[0], (pl.ds(0, n),)).wait()
        total = ar[kind, stage, 0]
        for i in range(1, n + 1):
            total = total + ar[kind, stage, i]
        return total

    load_h[1].start()
    pl.semaphore_wait(barrier, len(greeted))
    ar_send(0, 0, counts[0:1])

    for e in range(2):
        load_w[e].wait()
    score_sum = jnp.zeros((8, E), jnp.float32)
    for c in range(HCH):
        rows = pl.ds(c * HROWS, HROWS)
        load_h[c].wait()
        if c + 2 < HCH:
            load_h[c + 2].start()
        share[rows, :] = jnp.dot(h[rows, :], w[...], preferred_element_type=jnp.float32)
        for r0 in range(c * HROWS, (c + 1) * HROWS, STRIP):
            rows = pl.ds(r0, STRIP)
            scores = jax.nn.sigmoid(share[rows, :])
            inverse = 1.0 / jnp.sum(scores, axis=1, keepdims=True)
            position = start_at + r0 + lax.broadcasted_iota(jnp.int32, (STRIP, 1), 0)
            valid = jnp.where(position < live, 1.0, 0.0)
            part = scores * inverse
            share[rows, :] = part
            part = part * valid
            coef[rows, :] = part * (1.0 - scores)
            score_sum = score_sum + part.reshape(STRIP // 8, 8, E).sum(axis=0)
        if c == 1:
            counts = ar_wait(0, 0)
            ar_send(0, 1, counts)
    counts = ar_wait(0, 1)
    ar_send(1, 0, jnp.sum(score_sum, axis=0, keepdims=True))

    tokens = live.astype(jnp.float32)
    fraction = E * counts / (TOPK * tokens)
    weights = LOSS_SCALE * fraction / tokens
    for r0 in range(0, ROWS, 128):
        rows = pl.ds(r0, 128)
        weighted = jnp.sum(weights * share[rows, :], axis=1, keepdims=True)
        grad = (weights - weighted) * coef[rows, :]
        high = grad.astype(jnp.bfloat16)
        ghi[rows, :] = high
        glo[rows, :] = (grad - high.astype(jnp.float32)).astype(jnp.bfloat16)

    def d2d(j):
        return pltpu.make_async_remote_copy(
            src_ref=snd.at[j], dst_ref=got.at[j], send_sem=d2d_s.at[j], recv_sem=d2d_r.at[j],
            device_id=other, device_id_type=MESH,
        )

    def first(p, k, r):
        return pltpu.make_async_remote_copy(
            src_ref=acc[p].at[r], dst_ref=rb[p].at[r], send_sem=one_s.at[p, r], recv_sem=one_r.at[p, r],
            device_id=cube[dimension(p, k)], device_id_type=MESH,
        )

    def second(p, k, j):
        where = (pl.ds(4 >> k, 4 >> k), j)
        return pltpu.make_async_remote_copy(
            src_ref=acc[p].at[where], dst_ref=rb[p].at[where], send_sem=two_s.at[p - 3, k, j],
            recv_sem=two_r.at[p - 3, k, j], device_id=cube[dimension(p, k)], device_id_type=MESH,
        )

    def straight(p, r):
        return pltpu.make_async_remote_copy(
            src_ref=acc[p].at[0, r], dst_ref=rb[p].at[0, r], send_sem=far_s.at[p], recv_sem=far_r.at[p],
            device_id=far[p // 3][r], device_id_type=MESH,
        )

    def all_straight(p):
        where = (0, pl.ds(1, 7))
        return pltpu.make_async_remote_copy(
            src_ref=acc[p].at[where], dst_ref=rb[p].at[where], send_sem=far_s.at[p], recv_sem=far_r.at[p],
            device_id=far[p // 3][1], device_id_type=MESH,
        )

    def final(i, where):
        return pltpu.make_async_remote_copy(
            src_ref=fin.at[(core, v) + where], dst_ref=fin.at[(core, v) + where], send_sem=fin_s.at[i],
            recv_sem=fin_r.at[i], device_id=(cube[5], cross, other)[i], device_id_type=MESH,
        )

    yhi, xhi = y // 2, x // 2
    ylo, xlo = (yhi + y) % 2, (xhi + x) % 2
    v = (zh + zlo) % 2

    def multiply(j):
        y_hi = (yhi + j // 4) % 2
        y_at = 2 * y_hi + (y_hi + ylo + (j // 2) % 2) % 2
        x_hi = (xhi + j) % 2
        start = (y_at * 2 + x_hi) * CHUNK
        for m in range(CHUNK // 128):
            part = h[:, pl.ds(pl.multiple_of(start + m * 128, 128), 128)]
            dims = (((0,), (0,)), ((), ()))
            made = lax.dot_general(part, ghi[...], dims, preferred_element_type=jnp.float32)
            made = made + lax.dot_general(part, glo[...], dims, preferred_element_type=jnp.float32)
            at = m * 128
            while at < (m + 1) * 128:
                to = min((at // HALF + 1) * HALF, (m + 1) * 128)
                piece = at // HALF
                b1 = (x_hi + piece // 4 + xlo) % 2
                b2 = (piece // 2 % 2 + zh) % 2
                b3 = (piece % 2 + v) % 2
                b = b1 * 4 + b2 * 2 + b3
                lo, size = at - piece * HALF, to - at
                own[j, b, lo : lo + size] = made[at - m * 128 : to - m * 128, :128]
                snd[j, b, lo : lo + size] = made[at - m * 128 : to - m * 128, 128:]
                at = to
        d2d(j).start()

    def gather(j):
        d2d(j).wait_recv()
        for b in range(8):
            total = own[j, b] + got[j, b]
            for s in range(6):
                acc[s][place(s, j, b)] = total[OFFSET[s] : OFFSET[s] + 8 * TILES[s]]
        for p in SECOND:
            second(p, 0, j).start()
        for p, bit in ((0, j // 4), (1, (j // 2) % 2), (2, j % 2)):

            @pl.when(bit == 1)
            def _(p=p):
                first(p, 0, turn(j, p)).start()

    def advance(p, r):
        total = acc[p][r]
        for source in SOURCES[r]:
            first(p, 0 if source >= 4 else 1 if source >= 2 else 2, source).wait_recv()
            total = total + rb[p][source]
        acc[p][r] = total
        if r > 0:
            first(p, 1 if r >= 2 else 2, r).start()
        else:
            for b in (7, 6, 5, 3, 4, 2, 1):
                straight(p, b).start()

    def step(i, carry):
        @pl.when(i < 8)
        def _():
            multiply(7 - i)

        @pl.when((i > 1) & (i < 10))
        def _():
            gather(9 - i)

        @pl.when(i == 7)
        def _():
            ar_send(1, 1, ar_wait(1, 0))

        for at in sorted({at for at, _, _ in EVENTS}):

            @pl.when(i == at)
            def _(at=at):
                for at_, p, r in EVENTS:
                    if at_ == at:
                        advance(p, r)

        @pl.when((i > 4) & (i < 13))
        def _():
            j = 12 - i
            for p in SECOND:
                second(p, 0, j).wait_recv()
                acc[p][0:4, j] = acc[p][0:4, j] + rb[p][4:8, j]
                second(p, 1, j).start()

        @pl.when((i > 7) & (i < 16))
        def _():
            j = 15 - i
            for p in SECOND:
                second(p, 1, j).wait_recv()
                acc[p][0:2, j] = acc[p][0:2, j] + rb[p][2:4, j]
                second(p, 2, j).start()

        @pl.when((i > 10) & (i < 19))
        def _():
            j = 18 - i
            for p in SECOND:
                second(p, 2, j).wait_recv()
                acc[p][0, j] = acc[p][0, j] + rb[p][1, j]

        for r in range(1, 8):

            @pl.when(i == 18 - r)
            def _(r=r):
                for p in SECOND:
                    straight(p, r).start()

        return carry

    lax.fori_loop(0, 19, step, 0)

    for half, pieces in enumerate((FIRST, SECOND)):
        for p in pieces:
            all_straight(p).wait_recv()
            total = acc[p][0, 0]
            for r in range(1, 8):
                total = total + rb[p][0, r]
            fin[core, v, OFFSET[p] : OFFSET[p] + 8 * TILES[p]] = total
            for i in range(3):
                final(i, (pl.ds(OFFSET[p], 8 * TILES[p]),)).start()

    score_sum = ar_wait(1, 1)
    mean_score = score_sum / tokens
    bal[0] = jnp.sum(fraction * mean_score)

    for p in FIRST:
        for r in range(1, 8):
            first(p, 0, r).wait_send()
    for p in SECOND:
        for k in range(3):
            for j in range(8):
                second(p, k, j).wait_send()
    for p in range(6):
        all_straight(p).wait_send()
    for j in range(8):
        d2d(j).wait_send()
    for i in range(3):
        final(i, ()).wait()
    for e in range(2):
        for half in range(2):
            out[half * HALF : (half + 1) * HALF, e * 128 : (e + 1) * 128] = fin[e, half]


def solution(mesh):
    def shards(hidden, router_weight, expert_index, lengths):
        any_space = pl.BlockSpec(memory_space=pltpu.HBM)
        pieces = [(8, 8, 8 * t, 128) for t in TILES]
        return pl.pallas_call(
            kernel,
            out_shape=(pltpu.VMEM((BLOCK, E), jnp.float32), jax.ShapeDtypeStruct((1,), jnp.float32)),
            in_specs=[any_space] * 4,
            out_specs=(pl.BlockSpec(memory_space=pltpu.VMEM), pl.BlockSpec(memory_space=pltpu.SMEM)),
            scratch_shapes=[
                pltpu.VMEM((ROWS, D), jnp.bfloat16),
                pltpu.VMEM((D, E), jnp.bfloat16),
                pltpu.VMEM((TOPK, ROWS), jnp.int32),
                pltpu.SMEM((1,), jnp.int32),
                pltpu.VMEM((ROWS, E), jnp.float32),
                pltpu.VMEM((ROWS, E), jnp.float32),
                pltpu.VMEM((ROWS, E), jnp.bfloat16),
                pltpu.VMEM((ROWS, E), jnp.bfloat16),
                pltpu.VMEM((8, 8, HALF, 128), jnp.float32),
                pltpu.VMEM((8, 8, HALF, 128), jnp.float32),
                pltpu.VMEM((8, 8, HALF, 128), jnp.float32),
                *[pltpu.VMEM(p, jnp.float32) for p in pieces],
                *[pltpu.VMEM(p, jnp.float32) for p in pieces],
                pltpu.VMEM((2, 2, HALF, 128), jnp.float32),
                pltpu.VMEM((2, 2, 8, 1, E), jnp.float32),
                pltpu.SemaphoreType.DMA((4 + HCH,)),
                pltpu.SemaphoreType.DMA((8,)),
                pltpu.SemaphoreType.DMA((8,)),
                pltpu.SemaphoreType.DMA((3, 8)),
                pltpu.SemaphoreType.DMA((3, 8)),
                pltpu.SemaphoreType.DMA((3, 3, 8)),
                pltpu.SemaphoreType.DMA((3, 3, 8)),
                pltpu.SemaphoreType.DMA((6,)),
                pltpu.SemaphoreType.DMA((6,)),
                pltpu.SemaphoreType.DMA((2, 2)),
                pltpu.SemaphoreType.DMA((2, 2)),
                pltpu.SemaphoreType.DMA((3,)),
                pltpu.SemaphoreType.DMA((3,)),
            ],
            compiler_params=pltpu.CompilerParams(
                collective_id=0, has_side_effects=True, vmem_limit_bytes=64487424
            ),
        )(hidden, router_weight, expert_index.T, lengths)

    return jax.shard_map(
        shards,
        mesh=mesh,
        in_specs=(P(("seq", "ctx"), None), P(), P(("seq", "ctx"), None), P("seq")),
        out_specs=(P("ctx", None), P("seq")),
        check_vma=False,
    )
```
